64 devices in a mesh: dp: 8 (over x, y, core), sp: 8 (over z).
Axes of the slice: x: 2, y: 2, z: 8, core: 2. Of those that a mesh axis runs over, the one named last changes fastest.
The devices are a block of a 4x4x8 slice.
Arguments:
- x: bfloat16 [16384, 6144], P(('dp', 'sp')), parts along dimension 0
- gain: bfloat16 [6144], replicated
- wq: bfloat16 [6144, 6144], replicated
- wk: bfloat16 [6144, 1024], replicated
- wv: bfloat16 [6144, 1024], replicated
- wo: bfloat16 [6144, 6144], replicated
Outputs:
- output: bfloat16 [16384, 6144], P(('dp', 'sp')), parts along dimension 0
There are 8 independent parts. The reference program is written for one: setup_inputs(seed, part) draws one part's arguments, and reference() takes and returns one part's arrays. A program takes and returns all parts, laid end to end along the dimension named above; an argument that names none is the same for every part.
All inputs are finite; a program needn't handle non-finite values.
Results may differ from the reference program's by a relative error of at most 0.012.
Values are sent between devices in bfloat16 or wider.
A program may use at most 768 MiB of HBM per device.

```python
import jax
import jax.numpy as jnp
from jax import lax

ROWS = 2048
D = 6144
HEADS = 48
KV_HEADS = 8
HEAD = 128
THETA = 10000


def setup_inputs(seed: int = 0, part: int = 0) -> dict:
    kx, kn, kq, kk, kv, ko = jax.random.split(jax.random.key(seed), 6)

    def weights(key, rows, columns):
        return jax.random.normal(key, (rows, columns), jnp.float32) * rows**-0.5

    drawn = {
        "x": jax.random.normal(jax.random.fold_in(kx, part), (ROWS, D), jnp.float32),
        "gain": 1 + 0.1 * jax.random.normal(kn, (D,), jnp.float32),
        "wq": 2 * weights(kq, D, HEADS * HEAD),
        "wk": 2 * weights(kk, D, KV_HEADS * HEAD),
        "wv": 4 * weights(kv, D, KV_HEADS * HEAD),
        "wo": weights(ko, HEADS * HEAD, D),
    }
    return {k: v.astype(jnp.bfloat16) for k, v in drawn.items()}


def normed(x, gain):
    wide = x.astype(jnp.float32)
    scale = lax.rsqrt(jnp.mean(wide * wide, -1, keepdims=True) + 1e-6)
    return (wide * scale * gain.astype(jnp.float32)).astype(jnp.bfloat16)


def turned(t, place, theta):
    half = t.shape[-1] // 2
    angle = place.astype(jnp.float32)[:, None] * theta ** (-jnp.arange(half, dtype=jnp.float32) / half)
    cos, sin = jnp.cos(angle)[:, None], jnp.sin(angle)[:, None]
    a, b = t[..., :half].astype(jnp.float32), t[..., half:].astype(jnp.float32)
    return jnp.concatenate([a * cos - b * sin, b * cos + a * sin], -1).astype(jnp.bfloat16)


def matmul(a, w):
    return jnp.dot(a, w, preferred_element_type=jnp.float32).astype(jnp.bfloat16)


def einsum(form, a, b):
    return jnp.einsum(form, a.astype(jnp.float32), b.astype(jnp.float32))


def attention(q, k, v):
    scores = einsum("tgsd,ugd->gstu", q, k) * q.shape[-1] ** -0.5
    token = jnp.arange(q.shape[0])
    scores = jnp.where(token[:, None] >= token, scores, -jnp.inf)
    weights = jax.nn.softmax(scores, -1).astype(jnp.bfloat16)
    return einsum("gstu,ugd->tgsd", weights, v).astype(jnp.bfloat16)


def reference(x, gain, wq, wk, wv, wo):
    a, place = normed(x, gain), jnp.arange(ROWS)
    q = turned(matmul(a, wq).reshape(ROWS, HEADS, HEAD), place, THETA).reshape(ROWS, KV_HEADS, -1, HEAD)
    k = turned(matmul(a, wk).reshape(ROWS, KV_HEADS, HEAD), place, THETA)
    v = matmul(a, wv).reshape(ROWS, KV_HEADS, HEAD)
    seen = attention(q, k, v).reshape(ROWS, HEADS * HEAD)
    return (x.astype(jnp.float32) + jnp.dot(seen, wo, preferred_element_type=jnp.float32)).astype(jnp.bfloat16)
```

```python
import functools

import jax
import jax.numpy as jnp
from jax import lax
from jax.experimental import pallas as pl
from jax.experimental.pallas import tpu as pltpu
from jax.sharding import PartitionSpec as P

HEAD = 128
THETA = 10000
LOG2E = 1.4426950408889634
HIDDEN = -2e30
SLOTS = 4
WIDE = 256
STRIP = 512
F32, BF16 = jnp.float32, jnp.bfloat16


def _dot(a, b, ca, cb):
    return lax.dot_general(a, b, (((ca,), (cb,)), ((), ())), preferred_element_type=F32)


def _layer(n, x_hbm, gain_ref, freq_ref, wq, wk, wv, wo, y_hbm, x_s, a_s, kv_s, q_s, acc_s, seen_s, wa_s, wo_s, cos_s, sin_s, top_s, mix_s,
           ssem, rsem, wasem, wosem, iosem):
    me = lax.axis_index("sp")
    own, width = x_s.shape
    kvh = kv_s.shape[1]
    g = q_s.shape[0] // kvh
    cols = g * own
    hops = n // 2
    pairs = kvh * HEAD // WIDE
    per = WIDE // HEAD
    qtiles = wq.shape[1] // WIDE
    ocols = wo_s.shape[2]
    otiles = width // ocols
    e = HEAD**-0.5 * LOG2E
    right, left = lax.rem(me + 1, n), lax.rem(me + n - 1, n)

    def a_copy(ref, tile, slot):
        return pltpu.make_async_copy(ref.at[:, pl.ds(pl.multiple_of(tile * WIDE, WIDE), WIDE)], wa_s.at[slot], wasem.at[slot])

    def o_copy(u):
        h, c = lax.div(u, otiles), lax.rem(u, otiles)
        rows = pl.ds(pl.multiple_of(h * g * HEAD, g * HEAD), g * HEAD)
        slot = lax.rem(u, SLOTS)
        return pltpu.make_async_copy(wo.at[rows, pl.ds(pl.multiple_of(c * ocols, ocols), ocols)], wo_s.at[slot], wosem.at[slot])

    def y_copy(c):
        at = pl.ds(pl.multiple_of(c * ocols, ocols), ocols)
        return pltpu.make_async_copy(x_s.at[:, at], y_hbm.at[:, at], iosem.at[c])

    def _remote(way, h, hop, block):
        view = kv_s.at[block, h, way] if hop == hops else kv_s.at[block, h]
        return pltpu.make_async_remote_copy(view, view, ssem.at[way, hop - 1, h], rsem.at[way, hop - 1, h],
                                            device_id={"sp": right if way == 0 else left}, device_id_type=pl.DeviceIdType.MESH)

    def put(way, h, hop):
        return _remote(way, h, hop, lax.rem(me + n - (hop - 1), n) if way == 0 else lax.rem(me + hop - 1, n))

    def got(way, h, hop):
        return _remote(way, h, hop, lax.rem(me + n - hop, n) if way == 0 else lax.rem(me + hop, n))

    def pass_on(h, hop):
        for way in range(2):
            got(way, h, hop - 1).wait_recv()
            put(way, h, hop).start()

    def pass_on_if(h, hop):
        @pl.when(h < kvh)
        def _():
            pass_on(h, hop)

    x_copy = pltpu.make_async_copy(x_hbm, x_s, iosem.at[otiles])
    x_copy.start()
    for i in range(SLOTS):
        a_copy(wk if i % 2 == 0 else wv, i // 2, i).start()

    barrier = pltpu.get_barrier_semaphore()
    for other in (left, right):
        pl.semaphore_signal(barrier, inc=1, device_id={"sp": other}, device_id_type=pl.DeviceIdType.MESH)

    place = (me * own + lax.broadcasted_iota(jnp.int32, (own, HEAD), 0)).astype(F32)
    angle = place * freq_ref[...]
    cos_s[...] = jnp.cos(angle)
    sin = jnp.sin(angle)
    sin_s[...] = jnp.where(lax.broadcasted_iota(jnp.int32, (own, HEAD), 1) < HEAD // 2, -sin, sin)

    def turned(t):
        t = t.astype(BF16).astype(F32)
        return (t * cos_s[...] + pltpu.roll(t, HEAD // 2, 1) * sin_s[...]).astype(BF16)

    x_copy.wait()
    gain = gain_ref[...].astype(F32)

    def norm(r, _):
        rows = pl.ds(pl.multiple_of(r * 16, 16), 16)
        wide = x_s[rows, :].astype(F32)
        scale = lax.rsqrt(jnp.mean(wide * wide, -1, keepdims=True) + 1e-6)
        a_s[rows, :] = (wide * scale * gain).astype(BF16)

    lax.fori_loop(0, own // 16, norm, None)

    def send_own(p):
        for i in range(per):
            for way in range(2):
                put(way, p * per + i, 1).start()

    def refill(p, slot, ref):
        later = p + SLOTS // 2

        @pl.when(later < pairs)
        def _():
            a_copy(ref, later, slot).start()

        @pl.when(later >= pairs)
        def _():
            a_copy(wq, 2 * (later - pairs) + (0 if ref is wk else 1), slot).start()

    def kv_pair(p, _):
        slot = 2 * lax.rem(p, SLOTS // 2)
        a_copy(wk, p, slot).wait()

        @pl.when(p == 1)
        def _():
            pl.semaphore_wait(barrier, 2)

        @pl.when(p > 0)
        def _():
            send_own(p - 1)

        t = _dot(a_s[...], wa_s[slot], 1, 0)
        for i in range(per):
            kv_s[me, p * per + i, 0] = turned(t[:, i * HEAD : (i + 1) * HEAD])
        refill(p, slot, wk)
        a_copy(wv, p, slot + 1).wait()
        t = _dot(a_s[...], wa_s[slot + 1], 1, 0)
        for i in range(per):
            kv_s[me, p * per + i, 1] = t[:, i * HEAD : (i + 1) * HEAD].astype(BF16)
        refill(p, slot + 1, wv)

    lax.fori_loop(0, pairs, kv_pair, None)

    def q_tile(t, _):
        slot = lax.rem(t, SLOTS)
        a_copy(wq, t, slot).wait()

        @pl.when(t == 0)
        def _():
            send_own(pairs - 1)

        @pl.when(t == qtiles - 8)
        def _():
            pass_on(0, 2)

        @pl.when(t == qtiles - 6)
        def _():
            pass_on(1, 2)

        r = _dot(a_s[...], wa_s[slot], 1, 0)
        for i in range(per):
            q_s[t * per + i] = turned(r[:, i * HEAD : (i + 1) * HEAD])
        at = pl.ds(pl.multiple_of(t * WIDE, WIDE), WIDE)
        acc_s[:, at] = x_s[:, at].astype(F32)

        @pl.when(t + SLOTS < qtiles)
        def _():
            a_copy(wq, t + SLOTS, slot).start()

        @pl.when(t >= qtiles - SLOTS)
        def _():
            o_copy(t - (qtiles - SLOTS)).start()

    lax.fori_loop(0, qtiles, q_tile, None)

    strips = range(0, cols, STRIP)
    query = lax.rem(lax.broadcasted_iota(jnp.int32, (own, STRIP), 1), own)
    causal = query >= lax.broadcasted_iota(jnp.int32, (own, STRIP), 0)

    def block(h, j, count, first):
        q = q_s[pl.ds(h * g, g)].reshape(cols, HEAD)
        keys = kv_s[pl.ds(j, count), h, 0].reshape(count * own, HEAD)
        values = kv_s[pl.ds(j, count), h, 1].reshape(count * own, HEAD)
        values = jnp.concatenate([values.T, jnp.ones((8, count * own), BF16)], axis=0)
        scores = [_dot(keys, q[at : at + STRIP], 1, 1) for at in strips]
        weights, keeps = [], []
        for at, s in zip(strips, scores):
            if first:
                s = jnp.where(causal, s, HIDDEN)
                top = s.max(axis=0, keepdims=True)
            else:
                old = top_s[:, at : at + STRIP]
                top = jnp.maximum(old, s.max(axis=0, keepdims=True))
                keeps.append(jnp.exp2((old - top) * e))
            top_s[:, at : at + STRIP] = top
            weights.append(jnp.exp2((s - top) * e).astype(BF16))
        for i, at in enumerate(strips):
            new = _dot(values, weights[i], 1, 0)
            mix_s[:, at : at + STRIP] = new if first else mix_s[:, at : at + STRIP] * keeps[i] + new

    def attend(h):
        block(h, me, 1, True)
        lax.fori_loop(0, lax.div(me, 2), lambda i, _: block(h, 2 * i, 2, False), None)

        @pl.when(lax.rem(me, 2) == 1)
        def _():
            block(h, me - 1, 1, False)

        for i in range(g):
            at = slice(i * own, (i + 1) * own)
            seen_s[:, i * HEAD : (i + 1) * HEAD] = (mix_s[:HEAD, at] * (1 / mix_s[HEAD : HEAD + 1, at])).T.astype(BF16)

    def head(h, _):
        got(0, h, hops).wait_recv()
        got(1, h, hops).wait_recv()
        attend(h)

        def out_tile(c, _):
            u = h * otiles + c

            @pl.when(c == 0)
            def _():
                pass_on_if(h + 4, 2)

            @pl.when(c == 1)
            def _():
                pass_on_if(h + 3, 3)

            o_copy(u).wait()
            at = pl.ds(pl.multiple_of(c * ocols, ocols), ocols)
            acc_s[:, at] += _dot(seen_s[...], wo_s[lax.rem(u, SLOTS)], 1, 0)

            @pl.when(u + SLOTS < kvh * otiles)
            def _():
                o_copy(u + SLOTS).start()

            @pl.when(h == kvh - 1)
            def _():
                x_s[:, at] = acc_s[:, at].astype(BF16)
                y_copy(c).start()

        lax.fori_loop(0, otiles, out_tile, None)
        pass_on_if(h + 2, 4)

    for h, hop in ((0, 3), (2, 2), (1, 3), (0, 4), (3, 2), (2, 3), (1, 4)):
        pass_on(h, hop)
    lax.fori_loop(0, kvh, head, None)

    def drain(h, _):
        for hop in range(1, hops + 1):
            for way in range(2):
                put(way, h, hop).wait_send()

    lax.fori_loop(0, kvh, drain, None)
    for c in range(otiles):
        y_copy(c).wait()


def solution(mesh):
    n = mesh.shape["sp"]

    def step(x, gain, wq, wk, wv, wo):
        own, width = x.shape
        kvh, heads = wk.shape[1] // HEAD, wq.shape[1] // HEAD
        g = heads // kvh
        half = HEAD // 2
        freq = THETA ** (-jnp.arange(half, dtype=F32) / half)
        freq = jnp.concatenate([freq, freq])[None]
        vmem, hbm = pl.BlockSpec(memory_space=pltpu.VMEM), pl.BlockSpec(memory_space=pl.ANY)
        ocols = width // 3
        return pl.pallas_call(
            functools.partial(_layer, n),
            out_shape=jax.ShapeDtypeStruct(x.shape, x.dtype),
            in_specs=[hbm, vmem, vmem, hbm, hbm, hbm, hbm],
            out_specs=hbm,
            scratch_shapes=[
                pltpu.VMEM((own, width), BF16),
                pltpu.VMEM((own, width), BF16),
                pltpu.VMEM((n, kvh, 2, own, HEAD), BF16),
                pltpu.VMEM((heads, own, HEAD), BF16),
                pltpu.VMEM((own, width), F32),
                pltpu.VMEM((own, g * HEAD), BF16),
                pltpu.VMEM((SLOTS, width, WIDE), BF16),
                pltpu.VMEM((SLOTS, g * HEAD, ocols), BF16),
                pltpu.VMEM((own, HEAD), F32),
                pltpu.VMEM((own, HEAD), F32),
                pltpu.VMEM((1, g * own), F32),
                pltpu.VMEM((HEAD + 8, g * own), F32),
                pltpu.SemaphoreType.DMA((2, n // 2, kvh)),
                pltpu.SemaphoreType.DMA((2, n // 2, kvh)),
                pltpu.SemaphoreType.DMA((SLOTS,)),
                pltpu.SemaphoreType.DMA((SLOTS,)),
                pltpu.SemaphoreType.DMA((4,)),
            ],
            compiler_params=pltpu.CompilerParams(collective_id=0, has_side_effects=True, vmem_limit_bytes=67043328),
            name="layer",
        )(x, gain[None], freq, wq, wk, wv, wo)

    tokens, whole = P(("dp", "sp"), None), P(None, None)
    return jax.shard_map(
        step,
        mesh=mesh,
        in_specs=(tokens, P(None), whole, whole, whole, whole),
        out_specs=tokens,
        check_vma=False,
    )
```

```python
import functools
import math

import jax
import jax.numpy as jnp
from jax import lax
from jax.experimental import pallas as pl
from jax.experimental.pallas import tpu as pltpu
from jax.sharding import PartitionSpec as P

HEAD = 128
THETA = 10000
LOG2E = 1.4426950408889634
HIDDEN = -2e30
SLOTS = 3
OSLOTS = 2
WIDE = 512
F32, BF16 = jnp.float32, jnp.bfloat16


def _dot(a, b, ca, cb):
    return lax.dot_general(a, b, (((ca,), (cb,)), ((), ())), preferred_element_type=F32)


def _layer(n, x_hbm, gain_ref, wq, wk, wv, wo, y_hbm, x_s, a_s, kv_s, q_s, acc_s, seen_s, wa_s, wo_s, cos_s, sin_s, top_s, mix_s, s0_s, s1_s,
           w1_s, keep_s, r_s, ssem, rsem, wasem, wosem, iosem):
    me = lax.axis_index("sp")
    own, width = x_s.shape
    kvh = kv_s.shape[1]
    g = q_s.shape[0] // kvh
    half = g // 2 * own
    hops = n // 2
    hw = WIDE // 2
    per = hw // HEAD
    tiles = kvh // per
    qtiles = wq.shape[1] // WIDE
    ocols = wo_s.shape[2]
    otiles = width // ocols
    e = HEAD**-0.5 * LOG2E
    right, left = lax.rem(me + 1, n), lax.rem(me + n - 1, n)

    def a_half(ref, at, slot, side):
        cols = pl.ds(side * hw, hw)
        return pltpu.make_async_copy(ref.at[:, pl.ds(pl.multiple_of(at * hw, hw), hw)], wa_s.at[slot, :, cols], wasem.at[slot, side])

    def kv_tile(p, slot):
        return a_half(wk, p, slot, 0), a_half(wv, p, slot, 1)

    def q_copies(t, slot):
        return a_half(wq, 2 * t, slot, 0), a_half(wq, 2 * t + 1, slot, 1)

    def start(copies):
        for c in copies:
            c.start()

    def wait(copies):
        for c in copies:
            c.wait()

    def o_copy(u):
        h, c = lax.div(u, otiles), lax.rem(u, otiles)
        rows = pl.ds(pl.multiple_of(h * g * HEAD, g * HEAD), g * HEAD)
        slot = lax.rem(u, OSLOTS)
        return pltpu.make_async_copy(wo.at[rows, pl.ds(pl.multiple_of(c * ocols, ocols), ocols)], wo_s.at[slot], wosem.at[slot])

    def y_copy(c):
        at = pl.ds(pl.multiple_of(c * ocols, ocols), ocols)
        return pltpu.make_async_copy(x_s.at[:, at], y_hbm.at[:, at], iosem.at[c])

    def _remote(way, h, hop, block):
        view = kv_s.at[block, h, way] if hop == hops else kv_s.at[block, h]
        return pltpu.make_async_remote_copy(view, view, ssem.at[way, hop - 1, h], rsem.at[way, hop - 1, h],
                                            device_id={"sp": right if way == 0 else left}, device_id_type=pl.DeviceIdType.MESH)

    def put(way, h, hop):
        return _remote(way, h, hop, lax.rem(me + n - (hop - 1), n) if way == 0 else lax.rem(me + hop - 1, n))

    def got(way, h, hop):
        return _remote(way, h, hop, lax.rem(me + n - hop, n) if way == 0 else lax.rem(me + hop, n))

    def pass_on(h, hop):
        for way in range(2):
            if hop > 1:
                with jax.named_scope(f"pass_wait{hop}"):
                    got(way, h, hop - 1).wait_recv()
            put(way, h, hop).start()

    def pass_on_if(h, hop):
        @pl.when(h < kvh)
        def _():
            pass_on(h, hop)

    x_copy = pltpu.make_async_copy(x_hbm, x_s, iosem.at[otiles])
    x_copy.start()
    barrier = pltpu.get_barrier_semaphore()
    for other in (left, right):
        pl.semaphore_signal(barrier, inc=1, device_id={"sp": other}, device_id_type=pl.DeviceIdType.MESH)

    lane = lax.broadcasted_iota(jnp.int32, (own, HEAD), 1)
    place = (me * own + lax.broadcasted_iota(jnp.int32, (own, HEAD), 0)).astype(F32)
    turn = lax.rem(lane, HEAD // 2).astype(F32) * (-2.0 / HEAD * math.log2(THETA))
    angle = place * jnp.exp2(turn)
    cos_s[...] = jnp.cos(angle)
    sin = jnp.sin(angle)
    sin_s[...] = jnp.where(lane < HEAD // 2, -sin, sin)

    def turned(t):
        t = t.astype(BF16).astype(F32)
        return (t * cos_s[...] + pltpu.roll(t, HEAD // 2, 1) * sin_s[...]).astype(BF16)

    with jax.named_scope("x_wait"):
        x_copy.wait()
    for p in range(SLOTS):
        start(kv_tile(p, p))
    gain = gain_ref[...].reshape(1, width).astype(F32)

    def norm(r, _):
        rows = pl.ds(pl.multiple_of(r * 64, 64), 64)
        wide = x_s[rows, :].astype(F32)
        scale = lax.rsqrt(jnp.mean(wide * wide, -1, keepdims=True) + 1e-6)
        a_s[rows, :] = (wide * scale * gain).astype(BF16)

    with jax.named_scope("norm"):
        lax.fori_loop(0, own // 64, norm, None)

    def kv_step(p, _):
        slot = lax.rem(p, SLOTS)
        with jax.named_scope("kv_wait"):
            wait(kv_tile(p, slot))

        @pl.when(p == 1)
        def _():
            pl.semaphore_wait(barrier, 2)
            pass_on(0, 1)
            pass_on(1, 1)

        @pl.when(p == 2)
        def _():
            pass_on(2, 1)

        t = _dot(a_s[...], wa_s[slot], 1, 0)
        for i in range(per):
            kv_s[me, p * per + i, 0] = turned(t[:, i * HEAD : (i + 1) * HEAD])
            kv_s[me, p * per + i, 1] = t[:, hw + i * HEAD : hw + (i + 1) * HEAD].astype(BF16)

        @pl.when(p + SLOTS < tiles)
        def _():
            start(kv_tile(p + SLOTS, slot))

        @pl.when(p + SLOTS >= tiles)
        def _():
            start(q_copies(p + SLOTS - tiles, slot))

    lax.fori_loop(0, tiles, kv_step, None)

    def q_turn(t):
        for i in range(2 * per):
            q_s[t * 2 * per + i] = turned(r_s[:, i * HEAD : (i + 1) * HEAD])

    def q_tile(t, _):
        slot = lax.rem(t + tiles, SLOTS)
        with jax.named_scope("wq_wait"):
            wait(q_copies(t, slot))

        @pl.when(t == 1)
        def _():
            pass_on(0, 2)
            pass_on(3, 1)

        @pl.when(t == 4)
        def _():
            pass_on(1, 2)
            pass_on(0, 3)

        @pl.when(t == 7)
        def _():
            pass_on(4, 1)
            pass_on(2, 2)

        @pl.when(t == 8)
        def _():
            pass_on(1, 3)

        @pl.when(t == 10)
        def _():
            pass_on(0, 4)

        q_turn(jnp.maximum(t - 1, 0))
        r_s[...] = _dot(a_s[...], wa_s[slot], 1, 0)
        at = pl.ds(pl.multiple_of(t * WIDE, WIDE), WIDE)
        acc_s[:, at] = x_s[:, at].astype(F32)

        @pl.when(t + SLOTS < qtiles)
        def _():
            start(q_copies(t + SLOTS, slot))

        @pl.when(t >= qtiles - OSLOTS)
        def _():
            o_copy(t - (qtiles - OSLOTS)).start()

    r_s[...] = jnp.zeros_like(r_s)
    lax.fori_loop(0, qtiles, q_tile, None)
    q_turn(qtiles - 1)

    def score(dst, h, j, side):
        q = q_s[pl.ds(h * g + side * (g // 2), g // 2)].reshape(half, HEAD)
        dst[...] = _dot(kv_s[j, h, 0], q, 1, 1)

    def soften(src, side, first):
        at = slice(side * half, (side + 1) * half)
        s = src[...]
        keep = None
        if first:
            query = lax.rem(lax.broadcasted_iota(jnp.int32, (own, half), 1), own)
            s = jnp.where(query >= lax.broadcasted_iota(jnp.int32, (own, half), 0), s, HIDDEN)
            top = s.max(axis=0, keepdims=True)
        else:
            old = top_s[:, at]
            top = jnp.maximum(old, s.max(axis=0, keepdims=True))
            keep = jnp.exp2((old - top) * e)
        top_s[:, at] = top
        return jnp.exp2((s - top) * e).astype(BF16), keep

    def mix(h, j, weights, keep, side):
        at = slice(side * half, (side + 1) * half)
        values = jnp.concatenate([kv_s[j, h, 1].T, jnp.ones((8, own), BF16)], axis=0)
        new = _dot(values, weights, 1, 0)
        mix_s[:, at] = new if keep is None else mix_s[:, at] * keep + new

    def step(h, before, j, after, first):
        if before is not None:
            mix(h, before, w1_s[...], keep_s[...], 1)
        score(s1_s, h, j, 1)
        weights, keep = soften(s0_s, 0, first)
        if after is not None:
            score(s0_s, h, after, 0)
        mix(h, j, weights, keep, 0)
        weights, keep = soften(s1_s, 1, first)
        w1_s[...] = weights
        keep_s[...] = jnp.zeros_like(keep_s) if first else keep

    far = (me >= hops).astype(jnp.int32)

    def nth(i):
        return jnp.clip(i + far * (i >= me - hops).astype(jnp.int32), 0, n - 1)

    def last(count):
        return jnp.where(count > 0, nth(count - 1), me)

    def early(h):
        score(s0_s, h, me, 0)
        count = me - far
        step(h, None, me, jnp.where(count > 0, nth(0), me), True)

        def rest(i, _):
            step(h, jnp.where(i > 0, nth(i - 1), me), nth(i), nth(jnp.minimum(i + 1, count - 1)), False)

        lax.fori_loop(0, count, rest, None)

    def late(h):
        @pl.when(far == 1)
        def _():
            score(s0_s, h, me - hops, 0)
            step(h, last(me - far), me - hops, None, False)

        mix(h, jnp.where(far == 1, me - hops, last(me - far)), w1_s[...], keep_s[...], 1)
        for i in range(g):
            at = slice(i * own, (i + 1) * own)
            seen_s[:, i * HEAD : (i + 1) * HEAD] = (mix_s[:HEAD, at] * (1 / mix_s[HEAD : HEAD + 1, at])).T.astype(BF16)

    def head(h, _):
        pass_on_if(h + 5, 1)
        pass_on_if(h + 3, 2)
        pass_on_if(h + 2, 3)
        with jax.named_scope("last_wait"):
            got(0, h, hops).wait_recv()
            got(1, h, hops).wait_recv()
        pass_on_if(h + 1, 4)
        with jax.named_scope("late"):
            late(h)

        def out_tile(c, _):
            u = h * otiles + c
            with jax.named_scope("wo_wait"):
                o_copy(u).wait()
            at = pl.ds(pl.multiple_of(c * ocols, ocols), ocols)
            acc_s[:, at] += _dot(seen_s[...], wo_s[lax.rem(u, OSLOTS)], 1, 0)

            @pl.when(u + OSLOTS < kvh * otiles)
            def _():
                o_copy(u + OSLOTS).start()

            @pl.when(h == kvh - 1)
            def _():
                y_hbm[:, at] = acc_s[:, at].astype(BF16)

        lax.fori_loop(0, otiles, out_tile, None)

        @pl.when(h + 1 < kvh)
        def _():
            with jax.named_scope("early"):
                early(h + 1)

    mix_s[...] = jnp.zeros_like(mix_s)
    with jax.named_scope("early"):
        early(0)
    lax.fori_loop(0, kvh, head, None)

    def drain(h, _):
        for hop in range(1, hops + 1):
            for way in range(2):
                put(way, h, hop).wait_send()

    with jax.named_scope("drain"):
        lax.fori_loop(0, kvh, drain, None)


def solution(mesh):
    n = mesh.shape["sp"]

    def step(x, gain, wq, wk, wv, wo):
        own, width = x.shape
        kvh, heads = wk.shape[1] // HEAD, wq.shape[1] // HEAD
        g = heads // kvh
        vmem, hbm = pl.BlockSpec(memory_space=pltpu.VMEM), pl.BlockSpec(memory_space=pl.ANY)
        ocols = width // 2
        return pl.pallas_call(
            functools.partial(_layer, n),
            out_shape=pltpu.MemorySpace.VMEM(x.shape, x.dtype),
            in_specs=[hbm, vmem, hbm, hbm, hbm, hbm],
            out_specs=vmem,
            scratch_shapes=[
                pltpu.VMEM((own, width), BF16),
                pltpu.VMEM((own, width), BF16),
                pltpu.VMEM((n, kvh, 2, own, HEAD), BF16),
                pltpu.VMEM((heads, own, HEAD), BF16),
                pltpu.VMEM((own, width), F32),
                pltpu.VMEM((own, g * HEAD), BF16),
                pltpu.VMEM((SLOTS, width, WIDE), BF16),
                pltpu.VMEM((OSLOTS, g * HEAD, ocols), BF16),
                pltpu.VMEM((own, HEAD), F32),
                pltpu.VMEM((own, HEAD), F32),
                pltpu.VMEM((1, g * own), F32),
                pltpu.VMEM((HEAD + 8, g * own), F32),
                pltpu.VMEM((own, g // 2 * own), F32),
                pltpu.VMEM((own, g // 2 * own), F32),
                pltpu.VMEM((own, g // 2 * own), BF16),
                pltpu.VMEM((1, g // 2 * own), F32),
                pltpu.VMEM((own, WIDE), F32),
                pltpu.SemaphoreType.DMA((2, n // 2, kvh)),
                pltpu.SemaphoreType.DMA((2, n // 2, kvh)),
                pltpu.SemaphoreType.DMA((SLOTS, 2)),
                pltpu.SemaphoreType.DMA((OSLOTS,)),
                pltpu.SemaphoreType.DMA((4,)),
            ],
            compiler_params=pltpu.CompilerParams(collective_id=0, has_side_effects=True, vmem_limit_bytes=60*2**20),
            name="layer",
        )(x, gain, wq, wk, wv, wo)

    tokens, whole = P(("dp", "sp"), None), P(None, None)
    return jax.shard_map(
        step,
        mesh=mesh,
        in_specs=(tokens, P(None), whole, whole, whole, whole),
        out_specs=tokens,
        check_vma=False,
    )
```

```python
import functools
import math

import jax
import jax.numpy as jnp
from jax import lax
from jax.experimental import pallas as pl
from jax.experimental.pallas import tpu as pltpu
from jax.sharding import PartitionSpec as P

HEAD = 128
THETA = 10000
LOG2E = 1.4426950408889634
HIDDEN = -2e30
SLOTS = 3
WIDE = 512
F32, BF16 = jnp.float32, jnp.bfloat16

AT_KV = {1: ((1, 1),), 2: ((2, 1),), 3: ((0, 1),)}
AT_Q = {1: ((4, 1),), 2: ((2, 2),), 4: ((0, 2),), 5: ((4, 2),), 7: ((1, 2),), 8: ((0, 3),), 10: ((3, 1),), 11: ((1, 3),)}
AT_FIRST = ((0, 4), (2, 3))
AT_HEAD = {0: ((3, 2),), 1: ((2, 4),), 2: ((5, 2),), 3: ((5, 3),), 4: ((5, 4), (6, 3)), 5: ((7, 3),), 6: ((7, 4),)}
AT_BLOCK = {0: ((1, 4), (5, 1), (6, 1)), 1: ((3, 3), (7, 1)), 2: ((3, 4), (4, 3), (6, 2)), 3: ((4, 4), (7, 2)), 5: ((6, 4),)}
AT_MID = {}


def _dot(a, b, ca, cb):
    return lax.dot_general(a, b, (((ca,), (cb,)), ((), ())), preferred_element_type=F32)


def _layer(n, x_hbm, gain_ref, wq, wk, wv, wo, y_ref, a_s, kv_s, q_s, acc_s, seen_s, wa_s, cos_s, sin_s, top_s, mix_s, last_top_s, last_mix_s,
           s0_s, s1_s, s2_s, w0_s, w1_s, w2_s, keep_s, r_s, ssem, rsem, wasem, wosem, xsem):
    me = lax.axis_index("sp")
    own, width = y_ref.shape
    kvh = kv_s.shape[1]
    g = q_s.shape[0] // kvh
    depth = g * HEAD
    hops = n // 2
    hw = WIDE // 2
    per = hw // HEAD
    tiles = kvh // per
    qtiles = wq.shape[1] // WIDE
    otiles = width // WIDE
    fits = width // depth
    pieces = xsem.shape[0]
    rows_x = own // pieces
    e = HEAD**-0.5 * LOG2E
    right, left = lax.rem(me + 1, n), lax.rem(me + n - 1, n)

    def a_half(ref, at, slot, side):
        cols = pl.ds(side * hw, hw)
        return pltpu.make_async_copy(ref.at[:, pl.ds(pl.multiple_of(at * hw, hw), hw)], wa_s.at[slot, :, cols], wasem.at[slot, side])

    def kv_tile(p, slot):
        return a_half(wk, p, slot, 0), a_half(wv, p, slot, 1)

    def q_copies(t, slot):
        return a_half(wq, 2 * t, slot, 0), a_half(wq, 2 * t + 1, slot, 1)

    def o_place(h, c):
        at = lax.rem(h, 2) * otiles + c
        return lax.div(at, fits), pl.ds(pl.multiple_of(lax.rem(at, fits) * depth, depth), depth)

    def o_copies(h):
        copies = []
        for c in range(otiles):
            slot, rows = o_place(h, c)
            source = wo.at[pl.ds(pl.multiple_of(h * depth, depth), depth), pl.ds(c * WIDE, WIDE)]
            copies.append(pltpu.make_async_copy(source, wa_s.at[slot, rows], wosem.at[lax.rem(h, 2), c]))
        return copies

    def x_copy(r):
        rows = pl.ds(pl.multiple_of(r * rows_x, rows_x), rows_x)
        return pltpu.make_async_copy(x_hbm.at[rows], y_ref.at[rows], xsem.at[r])

    def start(copies):
        for c in copies:
            c.start()

    def wait(copies):
        for c in copies:
            c.wait()

    def _remote(way, h, hop, block):
        view = kv_s.at[block, h, way] if hop == hops else kv_s.at[block, h]
        return pltpu.make_async_remote_copy(view, view, ssem.at[way, hop - 1, h], rsem.at[way, hop - 1, h],
                                            device_id={"sp": right if way == 0 else left}, device_id_type=pl.DeviceIdType.MESH)

    def put(way, h, hop):
        return _remote(way, h, hop, lax.rem(me + n - (hop - 1), n) if way == 0 else lax.rem(me + hop - 1, n))

    def got(way, h, hop):
        return _remote(way, h, hop, lax.rem(me + n - hop, n) if way == 0 else lax.rem(me + hop, n))

    def gets(way, hop):
        return me >= hop if way == 0 else lax.rem(me + hop, n) < hops

    def puts(way, hop):
        return (me >= hop - 1) & (me < n - 1) if way == 0 else lax.rem(me + hop - 1, n) < hops

    def take(way, h, hop):
        @pl.when(gets(way, hop))
        def _():
            with jax.named_scope(f"wait{hop}"):
                got(way, h, hop).wait_recv()

    def pass_on(h, hop):
        for way in range(2):
            if hop > 1:
                take(way, h, hop - 1)

            @pl.when(puts(way, hop))
            def _():
                put(way, h, hop).start()

    def pass_at(table, now):
        for at, sends in table.items():
            @pl.when(now == at)
            def _(sends=sends):
                for h, hop in sends:
                    pass_on(h, hop)

    for r in range(pieces):
        x_copy(r).start()
    barrier = pltpu.get_barrier_semaphore()
    for other in (left, right):
        pl.semaphore_signal(barrier, inc=1, device_id={"sp": other}, device_id_type=pl.DeviceIdType.MESH)

    lane = lax.broadcasted_iota(jnp.int32, (own, HEAD), 1)
    place = (me * own + lax.broadcasted_iota(jnp.int32, (own, HEAD), 0)).astype(F32)
    turn = lax.rem(lane, HEAD // 2).astype(F32) * (-2.0 / HEAD * math.log2(THETA))
    angle = place * jnp.exp2(turn)
    cos_s[...] = jnp.cos(angle)
    sin = jnp.sin(angle)
    sin_s[...] = jnp.where(lane < HEAD // 2, -sin, sin)
    start(kv_tile(0, 0))

    def turned(t):
        t = t.astype(BF16).astype(F32)
        return (t * cos_s[...] + pltpu.roll(t, HEAD // 2, 1) * sin_s[...]).astype(BF16)

    def norm_scale(r, _):
        rows = pl.ds(pl.multiple_of(r * rows_x, rows_x), rows_x)
        x_copy(r).wait()
        total = jnp.zeros((rows_x, HEAD), F32)
        for c in range(0, width, HEAD):
            wide = y_ref[rows, c : c + HEAD].astype(F32)
            total += wide * wide
        scale = lax.rsqrt(jnp.sum(total, -1, keepdims=True) * (1 / width) + 1e-6)
        r_s[rows, :HEAD] = jnp.broadcast_to(scale, (rows_x, HEAD))

    gain = gain_ref[...].reshape(1, width).astype(F32)

    def norm(r, _):
        rows = pl.ds(pl.multiple_of(r * 32, 32), 32)
        scale = r_s[rows, :HEAD]
        for c in range(0, width, HEAD):
            a_s[rows, c : c + HEAD] = (y_ref[rows, c : c + HEAD].astype(F32) * scale * gain[:, c : c + HEAD]).astype(BF16)

    with jax.named_scope("norm_scale"):
        lax.fori_loop(0, pieces, norm_scale, None)
    start(kv_tile(1, 1))
    with jax.named_scope("norm"):
        lax.fori_loop(0, own // 32, norm, None)
    for p in range(2, SLOTS):
        start(kv_tile(p, p))

    def kv_step(p, _):
        slot = lax.rem(p, SLOTS)
        with jax.named_scope("kv_wait"):
            wait(kv_tile(p, slot))

        @pl.when(p == 1)
        def _():
            pl.semaphore_wait(barrier, 2)

        pass_at(AT_KV, p)
        t = _dot(a_s[...], wa_s[slot], 1, 0)
        for i in range(per):
            kv_s[me, p * per + i, 0] = turned(t[:, i * HEAD : (i + 1) * HEAD])
            v = t[:, hw + i * HEAD : hw + (i + 1) * HEAD].astype(BF16)
            for at in range(0, own, HEAD):
                kv_s[me, p * per + i, 1, at : at + HEAD] = v[at : at + HEAD].T

        @pl.when(p + SLOTS < tiles)
        def _():
            start(kv_tile(p + SLOTS, slot))

        @pl.when(p + SLOTS >= tiles)
        def _():
            start(q_copies(p + SLOTS - tiles, slot))

    lax.fori_loop(0, tiles, kv_step, None)

    def q_turn(t):
        for i in range(2 * per):
            q_s[t * 2 * per + i] = turned(r_s[:, i * HEAD : (i + 1) * HEAD]).T

    def q_tile(t, _):
        slot = lax.rem(t + tiles, SLOTS)
        with jax.named_scope("wq_wait"):
            wait(q_copies(t, slot))

        pass_at(AT_Q, t)
        q_turn(jnp.maximum(t - 1, 0))
        r_s[...] = _dot(a_s[...], wa_s[slot], 1, 0)
        at = pl.ds(pl.multiple_of(t * WIDE, WIDE), WIDE)
        acc_s[:, at] = y_ref[:, at].astype(F32)

        @pl.when(t + SLOTS < qtiles)
        def _():
            start(q_copies(t + SLOTS, slot))

    r_s[...] = jnp.zeros_like(r_s)
    lax.fori_loop(0, qtiles, q_tile, None)
    start(o_copies(0))
    q_turn(qtiles - 1)

    bufs = (s0_s, w0_s, 0), (s1_s, w1_s, 1)
    end = s2_s, w2_s, 2
    parts = range(g)

    def here(i):
        return slice(i * own, (i + 1) * own)

    def score(to, h, j):
        for i in parts:
            to[0][:, here(i)] = _dot(kv_s[j, h, 0], q_s[h * g + i], 1, 0)

    def soften(of, seen, tops, new_tops):
        for i in parts:
            s = of[0][:, here(i)]
            if seen is None:
                s = jnp.where(lax.broadcasted_iota(jnp.int32, s.shape, 1) >= lax.broadcasted_iota(jnp.int32, s.shape, 0), s, HIDDEN)
                top = level = s.max(axis=0, keepdims=True)
            else:
                old = tops[:, here(i)]
                top = level = jnp.maximum(old, s.max(axis=0, keepdims=True))
                top, level = jnp.where(seen, top, old), jnp.where(seen, top, -HIDDEN)
                keep_s[of[2] : of[2] + 1, here(i)] = jnp.exp2((old - top) * e)
            if new_tops is not None:
                new_tops[:, here(i)] = top
            of[1][:, here(i)] = jnp.exp2((s - level) * e).astype(BF16)

    def mixed(by, h, j, old, i):
        values = jnp.concatenate([kv_s[j, h, 1, at : at + HEAD] for at in range(0, own, HEAD)], axis=1)
        new = _dot(jnp.concatenate([values, jnp.ones((8, own), BF16)], axis=0), by[1][:, here(i)], 1, 0)
        return new if old is None else old[:, here(i)] * keep_s[by[2] : by[2] + 1, here(i)] + new

    far = (me >= hops).astype(jnp.int32)
    count = me - far
    most = n - 2

    def nth(i):
        return jnp.where(i <= count, jnp.clip(i - 1 + far * (i > me - hops).astype(jnp.int32), 0, n - 1), me) if i else me

    def late(h, step):
        at = jnp.where(far == 1, lax.rem(me + hops, n), me)
        if step == 0:
            score(end, h, at)
        elif step == 1:
            soften(end, far == 1, last_top_s, None)
        else:
            for i in parts:
                o = mixed(end, h, at, last_mix_s, i)
                seen_s[:, i * HEAD : (i + 1) * HEAD] = (o[:HEAD] * (1 / o[HEAD : HEAD + 1])).T.astype(BF16)

    def project(h, c, last):
        slot, rows = o_place(h, c)
        at = slice(c * WIDE, (c + 1) * WIDE)
        y = acc_s[:, at] + _dot(seen_s[...], wa_s[slot, rows], 1, 0)
        if last:
            y_ref[:, at] = y.astype(BF16)
        else:
            acc_s[:, at] = y

    def early(h, between=lambda k: None):
        score(bufs[0], h, me)
        between(0)
        for k in range(most + 1):
            of, other = bufs[k % 2], bufs[1 - k % 2]
            soften(of, k <= count if k else None, top_s, last_top_s if k == most else top_s)
            if k < most:
                score(other, h, nth(k + 1))
            if k:
                for i in parts:
                    mix_s[:, here(i)] = mixed(other, h, nth(k - 1), mix_s if k > 1 else None, i)
            between(k + 1)
        for i in parts:
            last_mix_s[:, here(i)] = mixed(bufs[most % 2], h, nth(most), mix_s, i)

    def head(h, _):
        pass_at(AT_HEAD, h)
        for way in range(2):
            take(way, h, hops)
        pass_at(AT_BLOCK, h)
        with jax.named_scope("wo_wait"):
            wait(o_copies(h))
        start(o_copies(h + 1))

        def between(k):
            if k < 3:
                late(h, k)
            for c in range(max(k - 3, 0) * otiles // (most - 1), max(k - 2, 0) * otiles // (most - 1)):
                project(h, c, False)

        with jax.named_scope("head"):
            early(h + 1, between)

    for h, hop in AT_FIRST:
        pass_on(h, hop)
    with jax.named_scope("early"):
        early(0)
    lax.fori_loop(0, kvh - 1, head, None)
    for way in range(2):
        take(way, kvh - 1, hops)
    wait(o_copies(kvh - 1))
    with jax.named_scope("end"):
        for k in range(3):
            late(kvh - 1, k)
        for c in range(otiles):
            project(kvh - 1, c, True)

    def drain(h, _):
        for hop in range(1, hops + 1):
            for way in range(2):
                @pl.when(puts(way, hop))
                def _():
                    put(way, h, hop).wait_send()

    with jax.named_scope("drain"):
        lax.fori_loop(0, kvh, drain, None)


def solution(mesh):
    n = mesh.shape["sp"]

    def step(x, gain, wq, wk, wv, wo):
        own, width = x.shape
        kvh, heads = wk.shape[1] // HEAD, wq.shape[1] // HEAD
        g = heads // kvh
        cols = g * own
        vmem, hbm = pl.BlockSpec(memory_space=pltpu.VMEM), pl.BlockSpec(memory_space=pl.ANY)
        return pl.pallas_call(
            functools.partial(_layer, n),
            out_shape=pltpu.MemorySpace.VMEM(x.shape, x.dtype),
            in_specs=[hbm, vmem, hbm, hbm, hbm, hbm],
            out_specs=vmem,
            scratch_shapes=[
                pltpu.VMEM((own, width), BF16),
                pltpu.VMEM((n, kvh, 2, own, HEAD), BF16),
                pltpu.VMEM((heads, HEAD, own), BF16),
                pltpu.VMEM((own, width), F32),
                pltpu.VMEM((own, g * HEAD), BF16),
                pltpu.VMEM((SLOTS, width, WIDE), BF16),
                pltpu.VMEM((own, HEAD), F32),
                pltpu.VMEM((own, HEAD), F32),
                pltpu.VMEM((1, cols), F32),
                pltpu.VMEM((HEAD + 8, cols), F32),
                pltpu.VMEM((1, cols), F32),
                pltpu.VMEM((HEAD + 8, cols), F32),
                pltpu.VMEM((own, cols), F32),
                pltpu.VMEM((own, cols), F32),
                pltpu.VMEM((own, cols), F32),
                pltpu.VMEM((own, cols), BF16),
                pltpu.VMEM((own, cols), BF16),
                pltpu.VMEM((own, cols), BF16),
                pltpu.VMEM((8, cols), F32),
                pltpu.VMEM((own, WIDE), F32),
                pltpu.SemaphoreType.DMA((2, n // 2, kvh)),
                pltpu.SemaphoreType.DMA((2, n // 2, kvh)),
                pltpu.SemaphoreType.DMA((SLOTS, 2)),
                pltpu.SemaphoreType.DMA((2, width // WIDE)),
                pltpu.SemaphoreType.DMA((4,)),
            ],
            compiler_params=pltpu.CompilerParams(collective_id=0, has_side_effects=True, vmem_limit_bytes=60 * 2**20),
            name="layer",
        )(x, gain, wq, wk, wv, wo)

    tokens, whole = P(("dp", "sp"), None), P(None, None)
    return jax.shard_map(
        step,
        mesh=mesh,
        in_specs=(tokens, P(None), whole, whole, whole, whole),
        out_specs=tokens,
        check_vma=False,
    )
```

```python
import functools
import math

import jax
import jax.numpy as jnp
from jax import lax
from jax.experimental import pallas as pl
from jax.experimental.pallas import tpu as pltpu
from jax.sharding import PartitionSpec as P

HEAD = 128
THETA = 10000
LOG2E = 1.4426950408889634
HIDDEN = -2e30
SLOTS = 3
WIDE = 512
F32, BF16 = jnp.float32, jnp.bfloat16
AT_KV = {1: ((0, 1),), 2: ((1, 1),), 3: ((2, 1),), 4: ((3, 1),), 5: ((4, 1),), 7: ((0, 2), (5, 1))}
AT_Q = {1: ((1, 2),), 7: ((0, 3), (6, 1), (2, 2)), 10: ((1, 3),)}
AT_FIRST = ((0, 4), (7, 1), (3, 2))
AT_HEAD = {1: ((3, 3),), 2: ((4, 3), (3, 4), (6, 2)), 3: ((5, 3), (4, 4), (7, 2)), 4: ((6, 3), (5, 4)), 5: ((7, 3), (6, 4)), 6: ((7, 4),)}
AT_BLOCK = {0: ((2, 3), (1, 4), (4, 2)), 1: ((2, 4), (5, 2))}
AT_MID = {}


def _dot(a, b, ca, cb):
    return lax.dot_general(a, b, (((ca,), (cb,)), ((), ())), preferred_element_type=F32)


def _layer(n, x_hbm, gain_ref, wq, wk, wv, wo, y_ref, a_s, kv_s, q_s, acc_s, seen_s, wa_s, cos_s, sin_s, top_s, mix_s, last_top_s, last_mix_s,
           s0_s, s1_s, s2_s, w0_s, w1_s, w2_s, keep_s, peak_s, r_s, ssem, rsem, wasem, wosem, xsem):
    me = lax.axis_index("sp")
    own, width = y_ref.shape
    kvh = kv_s.shape[1]
    g = q_s.shape[0] // kvh
    depth = g * HEAD
    hops = n // 2
    per = WIDE // HEAD
    qtiles = wq.shape[1] // WIDE
    otiles = width // WIDE
    fits = width // depth
    pieces = xsem.shape[0]
    rows_x = own // pieces
    e = HEAD**-0.5 * LOG2E
    right, left = lax.rem(me + 1, n), lax.rem(me + n - 1, n)

    def columns(ref, at, many, slot, side):
        source = ref.at[:, pl.ds(pl.multiple_of(at * many, many), many)]
        return pltpu.make_async_copy(source, wa_s.at[slot, :, pl.ds(side * many, many)], wasem.at[slot, side])

    def kv_tile(h, slot):
        return columns(wk, h, HEAD, slot, 0), columns(wv, h, HEAD, slot, 1)

    def q_copies(t, slot):
        return columns(wq, 2 * t, WIDE // 2, slot, 0), columns(wq, 2 * t + 1, WIDE // 2, slot, 1)

    def o_place(h, c):
        at = lax.rem(h, 2) * otiles + c
        return lax.div(at, fits), pl.ds(pl.multiple_of(lax.rem(at, fits) * depth, depth), depth)

    def o_copies(h):
        copies = []
        for c in range(otiles):
            slot, rows = o_place(h, c)
            source = wo.at[pl.ds(pl.multiple_of(h * depth, depth), depth), pl.ds(c * WIDE, WIDE)]
            copies.append(pltpu.make_async_copy(source, wa_s.at[slot, rows], wosem.at[lax.rem(h, 2), c]))
        return copies

    def x_copy(r):
        rows = pl.ds(pl.multiple_of(r * rows_x, rows_x), rows_x)
        return pltpu.make_async_copy(x_hbm.at[rows], y_ref.at[rows], xsem.at[r])

    def start(copies):
        for c in copies:
            c.start()

    def wait(copies):
        for c in copies:
            c.wait()

    def _remote(way, h, hop, block):
        view = kv_s.at[block, h, way] if hop == hops else kv_s.at[block, h]
        return pltpu.make_async_remote_copy(view, view, ssem.at[way, hop - 1, h], rsem.at[way, hop - 1, h],
                                            device_id={"sp": right if way == 0 else left}, device_id_type=pl.DeviceIdType.MESH)

    def put(way, h, hop):
        return _remote(way, h, hop, lax.rem(me + n - (hop - 1), n) if way == 0 else lax.rem(me + hop - 1, n))

    def got(way, h, hop):
        return _remote(way, h, hop, lax.rem(me + n - hop, n) if way == 0 else lax.rem(me + hop, n))

    def gets(way, hop):
        return me >= hop if way == 0 else lax.rem(me + hop, n) < hops

    def puts(way, hop):
        return (me >= hop - 1) & (me < n - 1) if way == 0 else lax.rem(me + hop - 1, n) < hops

    def take(way, h, hop):
        @pl.when(gets(way, hop))
        def _():
            with jax.named_scope(f"wait{hop}"):
                got(way, h, hop).wait_recv()

    def pass_on(h, hop):
        for way in range(2):
            if hop > 1:
                take(way, h, hop - 1)

            @pl.when(puts(way, hop))
            def _():
                put(way, h, hop).start()

    def pass_at(table, now):
        for at, sends in table.items():
            @pl.when(now == at)
            def _(sends=sends):
                for h, hop in sends:
                    pass_on(h, hop)

    for r in range(pieces):
        x_copy(r).start()
    start(kv_tile(0, 0))
    barrier = pltpu.get_barrier_semaphore()
    for other in (left, right):
        pl.semaphore_signal(barrier, inc=1, device_id={"sp": other}, device_id_type=pl.DeviceIdType.MESH)

    lane = lax.broadcasted_iota(jnp.int32, (own, HEAD), 1)
    place = (me * own + lax.broadcasted_iota(jnp.int32, (own, HEAD), 0)).astype(F32)
    turn = lax.rem(lane, HEAD // 2).astype(F32) * (-2.0 / HEAD * math.log2(THETA))
    angle = place * jnp.exp2(turn)
    cos_s[...] = jnp.cos(angle)
    sin = jnp.sin(angle)
    sin_s[...] = jnp.where(lane < HEAD // 2, -sin, sin)
    start(kv_tile(1, 1))

    def turned(t):
        t = t.astype(BF16).astype(F32)
        return (t * cos_s[...] + pltpu.roll(t, HEAD // 2, 1) * sin_s[...]).astype(BF16)

    def norm_scale(r, _):
        rows = pl.ds(pl.multiple_of(r * rows_x, rows_x), rows_x)
        x_copy(r).wait()
        total = jnp.zeros((rows_x, HEAD), F32)
        for c in range(0, width, HEAD):
            wide = y_ref[rows, c : c + HEAD].astype(F32)
            total += wide * wide
        scale = lax.rsqrt(jnp.sum(total, -1, keepdims=True) * (1 / width) + 1e-6)
        r_s[rows, :HEAD] = jnp.broadcast_to(scale, (rows_x, HEAD))

    gain = gain_ref[...].reshape(1, width).astype(F32)

    def norm(r, _):
        rows = pl.ds(pl.multiple_of(r * 32, 32), 32)
        scale = r_s[rows, :HEAD]
        for c in range(0, width, HEAD):
            a_s[rows, c : c + HEAD] = (y_ref[rows, c : c + HEAD].astype(F32) * scale * gain[:, c : c + HEAD]).astype(BF16)

    with jax.named_scope("norm_scale"):
        lax.fori_loop(0, pieces, norm_scale, None)
    for p in range(2, SLOTS):
        start(kv_tile(p, p))
    with jax.named_scope("norm"):
        lax.fori_loop(0, own // 32, norm, None)

    def kv_step(p, _):
        slot = lax.rem(p, SLOTS)
        with jax.named_scope("kv_wait"):
            wait(kv_tile(p, slot))

        @pl.when(p == 1)
        def _():
            pl.semaphore_wait(barrier, 2)

        pass_at(AT_KV, p)
        t = _dot(a_s[...], wa_s[slot, :, : 2 * HEAD], 1, 0)
        kv_s[me, p, 0] = turned(t[:, :HEAD])
        v = t[:, HEAD:].astype(BF16)
        for at in range(0, own, HEAD):
            kv_s[me, p, 1, at : at + HEAD] = v[at : at + HEAD].T

        @pl.when(p + SLOTS < kvh)
        def _():
            start(kv_tile(p + SLOTS, slot))

        @pl.when(p + SLOTS >= kvh)
        def _():
            start(q_copies(p + SLOTS - kvh, slot))

    lax.fori_loop(0, kvh, kv_step, None)

    def q_turn(t):
        for i in range(per):
            q_s[t * per + i] = turned(r_s[:, i * HEAD : (i + 1) * HEAD]).T

    def q_tile(t, _):
        slot = lax.rem(t + kvh, SLOTS)
        with jax.named_scope("wq_wait"):
            wait(q_copies(t, slot))

        pass_at(AT_Q, t)
        q_turn(jnp.maximum(t - 1, 0))
        r_s[...] = _dot(a_s[...], wa_s[slot], 1, 0)
        at = pl.ds(pl.multiple_of(t * WIDE, WIDE), WIDE)
        acc_s[:, at] = y_ref[:, at].astype(F32)

        @pl.when(t + SLOTS < qtiles)
        def _():
            start(q_copies(t + SLOTS, slot))

    r_s[...] = jnp.zeros_like(r_s)
    lax.fori_loop(0, qtiles, q_tile, None)
    start(o_copies(0))
    q_turn(qtiles - 1)

    bufs = (s0_s, w0_s, 0), (s1_s, w1_s, 1)
    end = s2_s, w2_s, 2
    parts = range(g)

    def here(i):
        return slice(i * own, (i + 1) * own)

    def score(to, h, j, own_block=False):
        for i in parts:
            s = _dot(kv_s[j, h, 0], q_s[h * g + i], 1, 0)
            if own_block:
                s = jnp.where(lax.broadcasted_iota(jnp.int32, s.shape, 1) >= lax.broadcasted_iota(jnp.int32, s.shape, 0), s, HIDDEN)
            to[0][:, here(i)] = s
            peak_s[to[2] : to[2] + 1, here(i)] = s.max(axis=0, keepdims=True)

    def soften(of, seen, tops, new_tops):
        for i in parts:
            peak = peak_s[of[2] : of[2] + 1, here(i)]
            if seen is None:
                top = level = peak
            else:
                old = tops[:, here(i)]
                top = jnp.where(seen, jnp.maximum(old, peak), old)
                level = jnp.where(seen, top, -HIDDEN)
                keep_s[of[2] : of[2] + 1, here(i)] = jnp.exp2((old - top) * e)
            if new_tops is not None:
                new_tops[:, here(i)] = top
            of[1][:, here(i)] = jnp.exp2((of[0][:, here(i)] - level) * e).astype(BF16)

    def mixed(by, h, j, old, i):
        values = jnp.concatenate([kv_s[j, h, 1, at : at + HEAD] for at in range(0, own, HEAD)], axis=1)
        new = _dot(jnp.concatenate([values, jnp.ones((8, own), BF16)], axis=0), by[1][:, here(i)], 1, 0)
        return new if old is None else old[:, here(i)] * keep_s[by[2] : by[2] + 1, here(i)] + new

    far = (me >= hops).astype(jnp.int32)
    count = me - far
    most = n - 2

    def nth(i):
        return jnp.where(i <= count, jnp.clip(i - 1 + far * (i > me - hops).astype(jnp.int32), 0, n - 1), me) if i else me

    def late(h, step):
        at = jnp.where(far == 1, lax.rem(me + hops, n), me)
        if step == 0:
            score(end, h, at)
        elif step == 1:
            soften(end, far == 1, last_top_s, None)
        else:
            for i in parts:
                o = mixed(end, h, at, last_mix_s, i)
                seen_s[:, i * HEAD : (i + 1) * HEAD] = (o[:HEAD] * (1 / o[HEAD : HEAD + 1])).T.astype(BF16)

    def project(h, c, last):
        slot, rows = o_place(h, c)
        at = slice(c * WIDE, (c + 1) * WIDE)
        y = acc_s[:, at] + _dot(seen_s[...], wa_s[slot, rows], 1, 0)
        if last:
            y_ref[:, at] = y.astype(BF16)
        else:
            acc_s[:, at] = y

    def early(h, between=lambda k: None):
        score(bufs[0], h, me, True)
        between(0)
        for k in range(most + 1):
            of, other = bufs[k % 2], bufs[1 - k % 2]
            soften(of, k <= count if k else None, top_s, last_top_s if k == most else top_s)
            if k < most:
                score(other, h, nth(k + 1))
            if k:
                for i in parts:
                    mix_s[:, here(i)] = mixed(other, h, nth(k - 1), mix_s if k > 1 else None, i)
            between(k + 1)
        for i in parts:
            last_mix_s[:, here(i)] = mixed(bufs[most % 2], h, nth(most), mix_s, i)

    def head(h, _):
        pass_at(AT_HEAD, h)
        for way in range(2):
            take(way, h, hops)
        pass_at(AT_BLOCK, h)
        with jax.named_scope("wo_wait"):
            wait(o_copies(h))
        start(o_copies(h + 1))

        def between(k):
            if k < 3:
                late(h, k)
            for c in range(max(k - 3, 0) * otiles // (most - 1), max(k - 2, 0) * otiles // (most - 1)):
                project(h, c, False)

        with jax.named_scope("head"):
            early(h + 1, between)

    for h, hop in AT_FIRST:
        pass_on(h, hop)
    with jax.named_scope("early"):
        early(0)
    lax.fori_loop(0, kvh - 1, head, None)
    for way in range(2):
        take(way, kvh - 1, hops)
    wait(o_copies(kvh - 1))
    with jax.named_scope("end"):
        for k in range(3):
            late(kvh - 1, k)
        for c in range(otiles):
            project(kvh - 1, c, True)

    def drain(h, _):
        for hop in range(1, hops + 1):
            for way in range(2):
                @pl.when(puts(way, hop))
                def _():
                    put(way, h, hop).wait_send()

    with jax.named_scope("drain"):
        lax.fori_loop(0, kvh, drain, None)


def solution(mesh):
    n = mesh.shape["sp"]

    def step(x, gain, wq, wk, wv, wo):
        own, width = x.shape
        kvh, heads = wk.shape[1] // HEAD, wq.shape[1] // HEAD
        g = heads // kvh
        cols = g * own
        vmem, hbm = pl.BlockSpec(memory_space=pltpu.VMEM), pl.BlockSpec(memory_space=pl.ANY)
        return pl.pallas_call(
            functools.partial(_layer, n),
            out_shape=pltpu.MemorySpace.VMEM(x.shape, x.dtype),
            in_specs=[hbm, vmem, hbm, hbm, hbm, hbm],
            out_specs=vmem,
            scratch_shapes=[
                pltpu.VMEM((own, width), BF16),
                pltpu.VMEM((n, kvh, 2, own, HEAD), BF16),
                pltpu.VMEM((heads, HEAD, own), BF16),
                pltpu.VMEM((own, width), F32),
                pltpu.VMEM((own, g * HEAD), BF16),
                pltpu.VMEM((SLOTS, width, WIDE), BF16),
                pltpu.VMEM((own, HEAD), F32),
                pltpu.VMEM((own, HEAD), F32),
                pltpu.VMEM((1, cols), F32),
                pltpu.VMEM((HEAD + 8, cols), F32),
                pltpu.VMEM((1, cols), F32),
                pltpu.VMEM((HEAD + 8, cols), F32),
                pltpu.VMEM((own, cols), F32),
                pltpu.VMEM((own, cols), F32),
                pltpu.VMEM((own, cols), F32),
                pltpu.VMEM((own, cols), BF16),
                pltpu.VMEM((own, cols), BF16),
                pltpu.VMEM((own, cols), BF16),
                pltpu.VMEM((8, cols), F32),
                pltpu.VMEM((8, cols), F32),
                pltpu.VMEM((own, WIDE), F32),
                pltpu.SemaphoreType.DMA((2, n // 2, kvh)),
                pltpu.SemaphoreType.DMA((2, n // 2, kvh)),
                pltpu.SemaphoreType.DMA((SLOTS, 2)),
                pltpu.SemaphoreType.DMA((2, width // WIDE)),
                pltpu.SemaphoreType.DMA((4,)),
            ],
            compiler_params=pltpu.CompilerParams(collective_id=0, has_side_effects=True, vmem_limit_bytes=60 * 2**20),
            name="layer",
        )(x, gain, wq, wk, wv, wo)

    tokens, whole = P(("dp", "sp"), None), P(None, None)
    return jax.shard_map(
        step,
        mesh=mesh,
        in_specs=(tokens, P(None), whole, whole, whole, whole),
        out_specs=tokens,
        check_vma=False,
    )
```

```python
import functools
import math

import jax
import jax.numpy as jnp
from jax import lax
from jax.experimental import pallas as pl
from jax.experimental.pallas import tpu as pltpu
from jax.sharding import PartitionSpec as P

HEAD = 128
THETA = 10000
LOG2E = 1.4426950408889634
HIDDEN = -2e30
SLOTS = 3
WIDE = 512
F32, BF16 = jnp.float32, jnp.bfloat16
AT_KV = {1: ((0, 1),), 2: ((1, 1),), 3: ((2, 1),), 4: ((3, 1),), 5: ((4, 1),), 7: ((0, 2), (5, 1))}
AT_Q = {1: ((1, 2),), 7: ((0, 3), (6, 1), (2, 2)), 10: ((1, 3),)}
AT_FIRST = ((0, 4), (7, 1), (3, 2))
AT_HEAD = {1: ((3, 3),), 2: ((4, 3), (3, 4), (6, 2)), 3: ((5, 3), (4, 4), (7, 2)), 4: ((6, 3), (5, 4)), 5: ((7, 3), (6, 4)), 6: ((7, 4),)}
AT_BLOCK = {0: ((2, 3), (1, 4), (4, 2)), 1: ((2, 4), (5, 2))}
AT_MID = {}


def _dot(a, b, ca, cb):
    return lax.dot_general(a, b, (((ca,), (cb,)), ((), ())), preferred_element_type=F32)


def _layer(n, x_hbm, gain_ref, wq, wk, wv, wo, y_ref, a_s, kv_s, q_s, acc_s, seen_s, seen2_s, wa_s, cos_s, sin_s, top_s, mix_s, last_top_s, last_mix_s,
           s0_s, s1_s, s2_s, w0_s, w1_s, w2_s, keep_s, peak_s, r_s, ssem, rsem, wasem, wosem, xsem):
    me = lax.axis_index("sp")
    own, width = y_ref.shape
    kvh = kv_s.shape[1]
    g = q_s.shape[0] // kvh
    depth = g * HEAD
    hops = n // 2
    per = WIDE // HEAD
    qtiles = wq.shape[1] // WIDE
    otiles = width // WIDE
    fits = width // depth
    pieces = xsem.shape[0]
    rows_x = own // pieces
    e = HEAD**-0.5 * LOG2E
    right, left = lax.rem(me + 1, n), lax.rem(me + n - 1, n)

    def columns(ref, at, many, slot, side):
        source = ref.at[:, pl.ds(pl.multiple_of(at * many, many), many)]
        return pltpu.make_async_copy(source, wa_s.at[slot, :, pl.ds(side * many, many)], wasem.at[slot, side])

    def kv_tile(h, slot):
        return columns(wk, h, HEAD, slot, 0), columns(wv, h, HEAD, slot, 1)

    def q_copies(t, slot):
        return columns(wq, 2 * t, WIDE // 2, slot, 0), columns(wq, 2 * t + 1, WIDE // 2, slot, 1)

    def o_place(h, c):
        at = lax.rem(h, 2) * otiles + c
        return lax.div(at, fits), pl.ds(pl.multiple_of(lax.rem(at, fits) * depth, depth), depth)

    def o_copies(h):
        copies = []
        for c in range(otiles):
            slot, rows = o_place(h, c)
            source = wo.at[pl.ds(pl.multiple_of(h * depth, depth), depth), pl.ds(c * WIDE, WIDE)]
            copies.append(pltpu.make_async_copy(source, wa_s.at[slot, rows], wosem.at[lax.rem(h, 2), c]))
        return copies

    def x_copy(r):
        rows = pl.ds(pl.multiple_of(r * rows_x, rows_x), rows_x)
        return pltpu.make_async_copy(x_hbm.at[rows], y_ref.at[rows], xsem.at[r])

    def start(copies):
        for c in copies:
            c.start()

    def wait(copies):
        for c in copies:
            c.wait()

    def _remote(way, h, hop, block):
        view = kv_s.at[block, h, way] if hop == hops else kv_s.at[block, h]
        return pltpu.make_async_remote_copy(view, view, ssem.at[way, hop - 1, h], rsem.at[way, hop - 1, h],
                                            device_id={"sp": right if way == 0 else left}, device_id_type=pl.DeviceIdType.MESH)

    def put(way, h, hop):
        return _remote(way, h, hop, lax.rem(me + n - (hop - 1), n) if way == 0 else lax.rem(me + hop - 1, n))

    def got(way, h, hop):
        return _remote(way, h, hop, lax.rem(me + n - hop, n) if way == 0 else lax.rem(me + hop, n))

    def gets(way, hop):
        return me >= hop if way == 0 else lax.rem(me + hop, n) < hops

    def puts(way, hop):
        return (me >= hop - 1) & (me < n - 1) if way == 0 else lax.rem(me + hop - 1, n) < hops

    def take(way, h, hop):
        @pl.when(gets(way, hop))
        def _():
            with jax.named_scope(f"wait{hop}"):
                got(way, h, hop).wait_recv()

    def pass_on(h, hop):
        for way in range(2):
            if hop > 1:
                take(way, h, hop - 1)

            @pl.when(puts(way, hop))
            def _():
                put(way, h, hop).start()

    def pass_at(table, now):
        for at, sends in table.items():
            if isinstance(now, int) and now != at:
                continue

            @pl.when(now == at)
            def _(sends=sends):
                for h, hop in sends:
                    pass_on(h, hop)

    for r in range(pieces):
        x_copy(r).start()
    start(kv_tile(0, 0))
    barrier = pltpu.get_barrier_semaphore()
    for other in (left, right):
        pl.semaphore_signal(barrier, inc=1, device_id={"sp": other}, device_id_type=pl.DeviceIdType.MESH)

    lane = lax.broadcasted_iota(jnp.int32, (own, HEAD), 1)
    place = (me * own + lax.broadcasted_iota(jnp.int32, (own, HEAD), 0)).astype(F32)
    turn = lax.rem(lane, HEAD // 2).astype(F32) * (-2.0 / HEAD * math.log2(THETA))
    angle = place * jnp.exp2(turn)
    cos_s[...] = jnp.cos(angle)
    sin = jnp.sin(angle)
    sin_s[...] = jnp.where(lane < HEAD // 2, -sin, sin)
    start(kv_tile(1, 1))

    def turned(t):
        t = t.astype(BF16).astype(F32)
        return (t * cos_s[...] + pltpu.roll(t, HEAD // 2, 1) * sin_s[...]).astype(BF16)

    def norm_scale(r, _):
        rows = pl.ds(pl.multiple_of(r * rows_x, rows_x), rows_x)
        x_copy(r).wait()
        total = jnp.zeros((rows_x, HEAD), F32)
        for c in range(0, width, HEAD):
            wide = y_ref[rows, c : c + HEAD].astype(F32)
            total += wide * wide
        scale = lax.rsqrt(jnp.sum(total, -1, keepdims=True) * (1 / width) + 1e-6)
        r_s[rows, :HEAD] = jnp.broadcast_to(scale, (rows_x, HEAD))

    gain = gain_ref[...].reshape(1, width).astype(F32)

    def norm(r, _):
        rows = pl.ds(pl.multiple_of(r * 64, 64), 64)
        scale = r_s[rows, :HEAD]
        for c in range(0, width, HEAD):
            a_s[rows, c : c + HEAD] = (y_ref[rows, c : c + HEAD].astype(F32) * scale * gain[:, c : c + HEAD]).astype(BF16)

    with jax.named_scope("norm_scale"):
        lax.fori_loop(0, pieces, norm_scale, None)
    for p in range(2, SLOTS):
        start(kv_tile(p, p))
    with jax.named_scope("norm"):
        lax.fori_loop(0, own // 64, norm, None)

    def kv_step(p, _):
        slot = lax.rem(p, SLOTS)
        with jax.named_scope("kv_wait"):
            wait(kv_tile(p, slot))

        @pl.when(p == 1)
        def _():
            pl.semaphore_wait(barrier, 2)

        pass_at(AT_KV, p)
        t = _dot(a_s[...], wa_s[slot, :, : 2 * HEAD], 1, 0)
        kv_s[me, p, 0] = turned(t[:, :HEAD])
        v = t[:, HEAD:].astype(BF16)
        for at in range(0, own, HEAD):
            kv_s[me, p, 1, at : at + HEAD] = v[at : at + HEAD].T

        @pl.when(p + SLOTS < kvh)
        def _():
            start(kv_tile(p + SLOTS, slot))

        @pl.when(p + SLOTS >= kvh)
        def _():
            start(q_copies(p + SLOTS - kvh, slot))

    lax.fori_loop(0, kvh, kv_step, None)

    def q_turn(t):
        for i in range(per):
            q_s[t * per + i] = turned(r_s[:, i * HEAD : (i + 1) * HEAD]).T

    def q_tile(t, _):
        slot = lax.rem(t + kvh, SLOTS)
        with jax.named_scope("wq_wait"):
            wait(q_copies(t, slot))

        pass_at(AT_Q, t)
        q_turn(jnp.maximum(t - 1, 0))
        r_s[...] = _dot(a_s[...], wa_s[slot], 1, 0)
        at = pl.ds(pl.multiple_of(t * WIDE, WIDE), WIDE)
        acc_s[:, at] = y_ref[:, at].astype(F32)

        @pl.when(t + SLOTS < qtiles)
        def _():
            start(q_copies(t + SLOTS, slot))

    r_s[...] = jnp.zeros_like(r_s)
    lax.fori_loop(0, qtiles, q_tile, None)
    start(o_copies(0))
    q_turn(qtiles - 1)

    bufs = (s0_s, w0_s, 0), (s1_s, w1_s, 1)
    end = s2_s, w2_s, 2
    parts = range(g)

    def here(i):
        return slice(i * own, (i + 1) * own)

    def score(to, h, j, own_block=False):
        for i in parts:
            s = _dot(kv_s[j, h, 0], q_s[h * g + i], 1, 0)
            if own_block:
                s = jnp.where(lax.broadcasted_iota(jnp.int32, s.shape, 1) >= lax.broadcasted_iota(jnp.int32, s.shape, 0), s, HIDDEN)
            to[0][:, here(i)] = s
            peak_s[to[2] : to[2] + 1, here(i)] = s.max(axis=0, keepdims=True)

    def soften(of, seen, tops, new_tops):
        for i in parts:
            peak = peak_s[of[2] : of[2] + 1, here(i)]
            if seen is None:
                top = level = peak
            else:
                old = tops[:, here(i)]
                top = jnp.where(seen, jnp.maximum(old, peak), old)
                level = jnp.where(seen, top, -HIDDEN)
                keep_s[of[2] : of[2] + 1, here(i)] = jnp.exp2((old - top) * e)
            if new_tops is not None:
                new_tops[:, here(i)] = top
            of[1][:, here(i)] = jnp.exp2((of[0][:, here(i)] - level) * e).astype(BF16)

    def mixed(by, h, j, old, i):
        values = jnp.concatenate([kv_s[j, h, 1, at : at + HEAD] for at in range(0, own, HEAD)], axis=1)
        new = _dot(jnp.concatenate([values, jnp.ones((8, own), BF16)], axis=0), by[1][:, here(i)], 1, 0)
        return new if old is None else old[:, here(i)] * keep_s[by[2] : by[2] + 1, here(i)] + new

    far = (me >= hops).astype(jnp.int32)
    count = me - far
    most = n - 2

    def nth(i):
        return jnp.where(i <= count, jnp.clip(i - 1 + far * (i > me - hops).astype(jnp.int32), 0, n - 1), me) if i else me

    def late(h, step, into=seen_s):
        at = jnp.where(far == 1, lax.rem(me + hops, n), me)
        if step == 0:
            score(end, h, at)
        elif step == 1:
            soften(end, far == 1, last_top_s, None)
        else:
            for i in parts:
                o = mixed(end, h, at, last_mix_s, i)
                into[:, i * HEAD : (i + 1) * HEAD] = (o[:HEAD] * (1 / o[HEAD : HEAD + 1])).T.astype(BF16)

    def project(h, c, last, of=seen_s):
        slot, rows = o_place(h, c)
        at = slice(c * WIDE, (c + 1) * WIDE)
        y = acc_s[:, at] + _dot(of[...], wa_s[slot, rows], 1, 0)
        if last:
            y_ref[:, at] = y.astype(BF16)
        else:
            acc_s[:, at] = y

    def early(h, between=lambda k: None):
        score(bufs[0], h, me, True)
        between(0)
        for k in range(most + 1):
            of, other = bufs[k % 2], bufs[1 - k % 2]
            soften(of, k <= count if k else None, top_s, last_top_s if k == most else top_s)
            if k < most:
                score(other, h, nth(k + 1))
            if k:
                for i in parts:
                    mix_s[:, here(i)] = mixed(other, h, nth(k - 1), mix_s if k > 1 else None, i)
            between(k + 1)
        for i in parts:
            last_mix_s[:, here(i)] = mixed(bufs[most % 2], h, nth(most), mix_s, i)

    def head(h, keep):
        pass_at(AT_HEAD, h)
        for way in range(2):
            take(way, h, hops)
        pass_at(AT_BLOCK, h)
        with jax.named_scope("wo_wait"):
            wait(o_copies(h))
        start(o_copies(h + 1))

        def between(k):
            if k < 3:
                late(h, k)
            for c in range(max(k - 3, 0) * (otiles - keep) // (most - 1), max(k - 2, 0) * (otiles - keep) // (most - 1)):
                project(h, c, False)

        with jax.named_scope("head"):
            early(h + 1, between)

    for h, hop in AT_FIRST:
        pass_on(h, hop)
    with jax.named_scope("early"):
        early(0)
    lax.fori_loop(0, kvh - 2, lambda h, _: head(h, 0), None)

    spare = otiles // 3
    head(kvh - 2, spare)
    for way in range(2):
        take(way, kvh - 1, hops)
    wait(o_copies(kvh - 1))
    with jax.named_scope("end"):
        for k in range(3):
            late(kvh - 1, k, seen2_s)
            for c in range(otiles - spare + k * spare // 3, otiles - spare + (k + 1) * spare // 3):
                project(kvh - 2, c, False)
        for c in range(otiles):
            project(kvh - 1, c, True, seen2_s)

    def drain(h, _):
        for hop in range(1, hops + 1):
            for way in range(2):
                @pl.when(puts(way, hop))
                def _():
                    put(way, h, hop).wait_send()

    with jax.named_scope("drain"):
        lax.fori_loop(0, kvh, drain, None)


def solution(mesh):
    n = mesh.shape["sp"]

    def step(x, gain, wq, wk, wv, wo):
        own, width = x.shape
        kvh, heads = wk.shape[1] // HEAD, wq.shape[1] // HEAD
        g = heads // kvh
        cols = g * own
        vmem, hbm = pl.BlockSpec(memory_space=pltpu.VMEM), pl.BlockSpec(memory_space=pl.ANY)
        return pl.pallas_call(
            functools.partial(_layer, n),
            out_shape=pltpu.MemorySpace.VMEM(x.shape, x.dtype),
            in_specs=[hbm, vmem, hbm, hbm, hbm, hbm],
            out_specs=vmem,
            scratch_shapes=[
                pltpu.VMEM((own, width), BF16),
                pltpu.VMEM((n, kvh, 2, own, HEAD), BF16),
                pltpu.VMEM((heads, HEAD, own), BF16),
                pltpu.VMEM((own, width), F32),
                pltpu.VMEM((own, g * HEAD), BF16),
                pltpu.VMEM((own, g * HEAD), BF16),
                pltpu.VMEM((SLOTS, width, WIDE), BF16),
                pltpu.VMEM((own, HEAD), F32),
                pltpu.VMEM((own, HEAD), F32),
                pltpu.VMEM((1, cols), F32),
                pltpu.VMEM((HEAD + 8, cols), F32),
                pltpu.VMEM((1, cols), F32),
                pltpu.VMEM((HEAD + 8, cols), F32),
                pltpu.VMEM((own, cols), F32),
                pltpu.VMEM((own, cols), F32),
                pltpu.VMEM((own, cols), F32),
                pltpu.VMEM((own, cols), BF16),
                pltpu.VMEM((own, cols), BF16),
                pltpu.VMEM((own, cols), BF16),
                pltpu.VMEM((8, cols), F32),
                pltpu.VMEM((8, cols), F32),
                pltpu.VMEM((own, WIDE), F32),
                pltpu.SemaphoreType.DMA((2, n // 2, kvh)),
                pltpu.SemaphoreType.DMA((2, n // 2, kvh)),
                pltpu.SemaphoreType.DMA((SLOTS, 2)),
                pltpu.SemaphoreType.DMA((2, width // WIDE)),
                pltpu.SemaphoreType.DMA((2,)),
            ],
            compiler_params=pltpu.CompilerParams(collective_id=0, has_side_effects=True, vmem_limit_bytes=60 * 2**20),
            name="layer",
        )(x, gain, wq, wk, wv, wo)

    tokens, whole = P(("dp", "sp"), None), P(None, None)
    return jax.shard_map(
        step,
        mesh=mesh,
        in_specs=(tokens, P(None), whole, whole, whole, whole),
        out_specs=tokens,
        check_vma=False,
    )
```

```python
import functools
import math

import jax
import jax.numpy as jnp
from jax import lax
from jax.experimental import pallas as pl
from jax.experimental.pallas import tpu as pltpu
from jax.sharding import PartitionSpec as P

HEAD = 128
THETA = 10000
LOG2E = 1.4426950408889634
HIDDEN = -2e30
SLOTS = 3
WIDE = 512
F32, BF16 = jnp.float32, jnp.bfloat16
AT_KV = {1: ((0, 1),), 2: ((1, 1),), 3: ((2, 1),), 4: ((3, 1),), 5: ((4, 1),), 7: ((0, 2), (5, 1))}
AT_Q = {1: ((1, 2),), 7: ((0, 3), (6, 1), (2, 2)), 10: ((1, 3),)}
AT_FIRST = ((0, 4), (7, 1), (3, 2))
AT_HEAD = {1: ((3, 3),), 2: ((4, 3), (3, 4), (6, 2)), 3: ((5, 3), (4, 4), (7, 2)), 4: ((6, 3), (5, 4)), 5: ((7, 3), (6, 4)), 6: ((7, 4),)}
AT_BLOCK = {0: ((2, 3), (1, 4), (4, 2)), 1: ((2, 4), (5, 2))}
AT_MID = {}


def _dot(a, b, ca, cb):
    return lax.dot_general(a, b, (((ca,), (cb,)), ((), ())), preferred_element_type=F32)


def _layer(n, x_hbm, gain_ref, wq, wk, wv, wo, y_ref, a_s, kv_s, q_s, acc_s, seen_s, seen2_s, wa_s, cos_s, sin_s, top_s, mix_s, last_top_s, last_mix_s,
           s0_s, s1_s, s2_s, w0_s, w1_s, w2_s, keep_s, peak_s, r_s, ssem, rsem, wasem, wosem, xsem):
    me = lax.axis_index("sp")
    own, width = y_ref.shape
    kvh = kv_s.shape[1]
    g = q_s.shape[0] // kvh
    depth = g * HEAD
    hops = n // 2
    per = WIDE // HEAD
    qtiles = wq.shape[1] // WIDE
    otiles = width // WIDE
    fits = width // depth
    pieces = xsem.shape[0]
    rows_x = own // pieces
    e = HEAD**-0.5 * LOG2E
    right, left = lax.rem(me + 1, n), lax.rem(me + n - 1, n)

    def columns(ref, at, many, slot, side):
        source = ref.at[:, pl.ds(pl.multiple_of(at * many, many), many)]
        return pltpu.make_async_copy(source, wa_s.at[slot, :, pl.ds(side * many, many)], wasem.at[slot, side])

    def kv_tile(h, slot):
        return columns(wk, h, HEAD, slot, 0), columns(wv, h, HEAD, slot, 1)

    def q_copies(t, slot):
        return columns(wq, 2 * t, WIDE // 2, slot, 0), columns(wq, 2 * t + 1, WIDE // 2, slot, 1)

    def o_place(h, c):
        at = lax.rem(h, 2) * otiles + c
        return lax.div(at, fits), pl.ds(pl.multiple_of(lax.rem(at, fits) * depth, depth), depth)

    def o_copies(h):
        copies = []
        for c in range(otiles):
            slot, rows = o_place(h, c)
            source = wo.at[pl.ds(pl.multiple_of(h * depth, depth), depth), pl.ds(c * WIDE, WIDE)]
            copies.append(pltpu.make_async_copy(source, wa_s.at[slot, rows], wosem.at[lax.rem(h, 2), c]))
        return copies

    def x_copy(r):
        rows = pl.ds(pl.multiple_of(r * rows_x, rows_x), rows_x)
        return pltpu.make_async_copy(x_hbm.at[rows], y_ref.at[rows], xsem.at[r])

    def start(copies):
        for c in copies:
            c.start()

    def wait(copies):
        for c in copies:
            c.wait()

    def _remote(way, h, hop, block):
        view = kv_s.at[block, h, way] if hop == hops else kv_s.at[block, h]
        return pltpu.make_async_remote_copy(view, view, ssem.at[way, hop - 1, h], rsem.at[way, hop - 1, h],
                                            device_id={"sp": right if way == 0 else left}, device_id_type=pl.DeviceIdType.MESH)

    def put(way, h, hop):
        return _remote(way, h, hop, lax.rem(me + n - (hop - 1), n) if way == 0 else lax.rem(me + hop - 1, n))

    def got(way, h, hop):
        return _remote(way, h, hop, lax.rem(me + n - hop, n) if way == 0 else lax.rem(me + hop, n))

    def gets(way, hop):
        return me >= hop if way == 0 else lax.rem(me + hop, n) < hops

    def puts(way, hop):
        return (me >= hop - 1) & (me < n - 1) if way == 0 else lax.rem(me + hop - 1, n) < hops

    def take(way, h, hop):
        @pl.when(gets(way, hop))
        def _():
            with jax.named_scope(f"wait{hop}"):
                got(way, h, hop).wait_recv()

    def pass_on(h, hop):
        for way in range(2):
            if hop > 1:
                take(way, h, hop - 1)

            @pl.when(puts(way, hop))
            def _():
                put(way, h, hop).start()

    def pass_at(table, now):
        for at, sends in table.items():
            if isinstance(now, int) and now != at:
                continue

            @pl.when(now == at)
            def _(sends=sends):
                for h, hop in sends:
                    pass_on(h, hop)

    for r in range(pieces):
        x_copy(r).start()
    start(kv_tile(0, 0))
    barrier = pltpu.get_barrier_semaphore()
    for other in (left, right):
        pl.semaphore_signal(barrier, inc=1, device_id={"sp": other}, device_id_type=pl.DeviceIdType.MESH)

    lane = lax.broadcasted_iota(jnp.int32, (own, HEAD), 1)
    place = (me * own + lax.broadcasted_iota(jnp.int32, (own, HEAD), 0)).astype(F32)
    turn = lax.rem(lane, HEAD // 2).astype(F32) * (-2.0 / HEAD * math.log2(THETA))
    angle = place * jnp.exp2(turn)
    cos_s[...] = jnp.cos(angle)
    sin = jnp.sin(angle)
    sin_s[...] = jnp.where(lane < HEAD // 2, -sin, sin)
    start(kv_tile(1, 1))

    def turned(t):
        t = t.astype(BF16).astype(F32)
        return (t * cos_s[...] + pltpu.roll(t, HEAD // 2, 1) * sin_s[...]).astype(BF16)

    def norm_scale(r, _):
        rows = pl.ds(pl.multiple_of(r * rows_x, rows_x), rows_x)
        x_copy(r).wait()
        total = jnp.zeros((rows_x, HEAD), F32)
        for c in range(0, width, HEAD):
            wide = y_ref[rows, c : c + HEAD].astype(F32)
            total += wide * wide
        scale = lax.rsqrt(jnp.sum(total, -1, keepdims=True) * (1 / width) + 1e-6)
        r_s[rows, :HEAD] = jnp.broadcast_to(scale, (rows_x, HEAD))

    gain = gain_ref[...].reshape(1, width).astype(F32)

    def norm(r, _):
        rows = pl.ds(pl.multiple_of(r * 64, 64), 64)
        scale = r_s[rows, :HEAD]
        for c in range(0, width, HEAD):
            a_s[rows, c : c + HEAD] = (y_ref[rows, c : c + HEAD].astype(F32) * scale * gain[:, c : c + HEAD]).astype(BF16)

    with jax.named_scope("norm_scale"):
        lax.fori_loop(0, pieces, norm_scale, None)
    for p in range(2, SLOTS):
        start(kv_tile(p, p))
    with jax.named_scope("norm"):
        lax.fori_loop(0, own // 64, norm, None)

    def kv_step(p, _):
        slot = lax.rem(p, SLOTS)
        with jax.named_scope("kv_wait"):
            wait(kv_tile(p, slot))

        @pl.when(p == 1)
        def _():
            pl.semaphore_wait(barrier, 2)

        pass_at(AT_KV, p)
        t = _dot(a_s[...], wa_s[slot, :, : 2 * HEAD], 1, 0)
        kv_s[me, p, 0] = turned(t[:, :HEAD])
        v = t[:, HEAD:].astype(BF16)
        for at in range(0, own, HEAD):
            kv_s[me, p, 1, at : at + HEAD] = v[at : at + HEAD].T

        @pl.when(p + SLOTS < kvh)
        def _():
            start(kv_tile(p + SLOTS, slot))

        @pl.when(p + SLOTS >= kvh)
        def _():
            start(q_copies(p + SLOTS - kvh, slot))

    lax.fori_loop(0, kvh, kv_step, None)

    def q_turn(t):
        for i in range(per):
            q_s[t * per + i] = turned(r_s[:, i * HEAD : (i + 1) * HEAD]).T

    def q_tile(t, _):
        slot = lax.rem(t + kvh, SLOTS)
        with jax.named_scope("wq_wait"):
            wait(q_copies(t, slot))

        pass_at(AT_Q, t)
        q_turn(jnp.maximum(t - 1, 0))
        r_s[...] = _dot(a_s[...], wa_s[slot], 1, 0)
        at = pl.ds(pl.multiple_of(t * WIDE, WIDE), WIDE)
        acc_s[:, at] = y_ref[:, at].astype(F32)

        @pl.when(t + SLOTS < qtiles)
        def _():
            start(q_copies(t + SLOTS, slot))

    r_s[...] = jnp.zeros_like(r_s)
    lax.fori_loop(0, qtiles, q_tile, None)
    start(o_copies(0))
    q_turn(qtiles - 1)

    bufs = (s0_s, w0_s, 0), (s1_s, w1_s, 1)
    end = s2_s, w2_s, 2
    parts = range(g)

    def here(i):
        return slice(i * own, (i + 1) * own)

    def score(to, h, j, own_block=False):
        for i in parts:
            s = _dot(kv_s[j, h, 0], q_s[h * g + i], 1, 0)
            if own_block:
                s = jnp.where(lax.broadcasted_iota(jnp.int32, s.shape, 1) >= lax.broadcasted_iota(jnp.int32, s.shape, 0), s, HIDDEN)
            to[0][:, here(i)] = s
            peak_s[to[2] : to[2] + 1, here(i)] = s.max(axis=0, keepdims=True)

    def soften(of, seen, tops, new_tops):
        for i in parts:
            peak = peak_s[of[2] : of[2] + 1, here(i)]
            if seen is None:
                top = level = peak
            else:
                old = tops[:, here(i)]
                top = jnp.where(seen, jnp.maximum(old, peak), old)
                level = jnp.where(seen, top, -HIDDEN)
                keep_s[of[2] : of[2] + 1, here(i)] = jnp.exp2((old - top) * e)
            if new_tops is not None:
                new_tops[:, here(i)] = top
            of[1][:, here(i)] = jnp.exp2((of[0][:, here(i)] - level) * e).astype(BF16)

    def mixed(by, h, j, old, i):
        values = jnp.concatenate([kv_s[j, h, 1, at : at + HEAD] for at in range(0, own, HEAD)], axis=1)
        new = _dot(jnp.concatenate([values, jnp.ones((8, own), BF16)], axis=0), by[1][:, here(i)], 1, 0)
        return new if old is None else old[:, here(i)] * keep_s[by[2] : by[2] + 1, here(i)] + new

    far = (me >= hops).astype(jnp.int32)
    count = me - far
    most = n - 2

    def nth(i):
        return jnp.where(i <= count, jnp.clip(i - 1 + far * (i > me - hops).astype(jnp.int32), 0, n - 1), me) if i else me

    def late(h, step, into=seen_s):
        at = jnp.where(far == 1, lax.rem(me + hops, n), me)
        if step == 0:
            score(end, h, at)
        elif step == 1:
            soften(end, far == 1, last_top_s, None)
        else:
            for i in parts:
                o = mixed(end, h, at, last_mix_s, i)
                into[:, i * HEAD : (i + 1) * HEAD] = (o[:HEAD] * (1 / o[HEAD : HEAD + 1])).T.astype(BF16)

    def project(h, c, last, of=seen_s):
        slot, rows = o_place(h, c)
        at = slice(c * WIDE, (c + 1) * WIDE)
        y = acc_s[:, at] + _dot(of[...], wa_s[slot, rows], 1, 0)
        if last:
            y_ref[:, at] = y.astype(BF16)
        else:
            acc_s[:, at] = y

    def early(h, between=lambda k: None):
        score(bufs[0], h, me, True)
        between(0)
        for k in range(most + 1):
            of, other = bufs[k % 2], bufs[1 - k % 2]
            soften(of, k <= count if k else None, top_s, last_top_s if k == most else top_s)
            if k < most:
                score(other, h, nth(k + 1))
            if k:
                for i in parts:
                    mix_s[:, here(i)] = mixed(other, h, nth(k - 1), mix_s if k > 1 else None, i)
            between(k + 1)
        for i in parts:
            last_mix_s[:, here(i)] = mixed(bufs[most % 2], h, nth(most), mix_s, i)

    def head(h, keep):
        pass_at(AT_HEAD, h)
        for way in range(2):
            take(way, h, hops)
        pass_at(AT_BLOCK, h)
        with jax.named_scope("wo_wait"):
            wait(o_copies(h))
        start(o_copies(h + 1))

        def between(k):
            for part in {0: (0, 1), 1: (2,)}.get(k, ()):
                late(h, part)
            for c in range(max(k - 2, 0) * (otiles - keep) // most, max(k - 1, 0) * (otiles - keep) // most):
                project(h, c, False)

        with jax.named_scope("head"):
            early(h + 1, between)

    for h, hop in AT_FIRST:
        pass_on(h, hop)
    with jax.named_scope("early"):
        early(0)
    lax.fori_loop(0, kvh - 2, lambda h, _: head(h, 0), None)

    spare = otiles // 3
    head(kvh - 2, spare)
    for way in range(2):
        take(way, kvh - 1, hops)
    wait(o_copies(kvh - 1))
    with jax.named_scope("end"):
        for k in range(3):
            late(kvh - 1, k, seen2_s)
            for c in range(otiles - spare + k * spare // 3, otiles - spare + (k + 1) * spare // 3):
                project(kvh - 2, c, False)
        for c in range(otiles):
            project(kvh - 1, c, True, seen2_s)

    def drain(h, _):
        for hop in range(1, hops + 1):
            for way in range(2):
                @pl.when(puts(way, hop))
                def _():
                    put(way, h, hop).wait_send()

    with jax.named_scope("drain"):
        lax.fori_loop(0, kvh, drain, None)


def solution(mesh):
    n = mesh.shape["sp"]

    def step(x, gain, wq, wk, wv, wo):
        own, width = x.shape
        kvh, heads = wk.shape[1] // HEAD, wq.shape[1] // HEAD
        g = heads // kvh
        cols = g * own
        vmem, hbm = pl.BlockSpec(memory_space=pltpu.VMEM), pl.BlockSpec(memory_space=pl.ANY)
        return pl.pallas_call(
            functools.partial(_layer, n),
            out_shape=pltpu.MemorySpace.VMEM(x.shape, x.dtype),
            in_specs=[hbm, vmem, hbm, hbm, hbm, hbm],
            out_specs=vmem,
            scratch_shapes=[
                pltpu.VMEM((own, width), BF16),
                pltpu.VMEM((n, kvh, 2, own, HEAD), BF16),
                pltpu.VMEM((heads, HEAD, own), BF16),
                pltpu.VMEM((own, width), F32),
                pltpu.VMEM((own, g * HEAD), BF16),
                pltpu.VMEM((own, g * HEAD), BF16),
                pltpu.VMEM((SLOTS, width, WIDE), BF16),
                pltpu.VMEM((own, HEAD), F32),
                pltpu.VMEM((own, HEAD), F32),
                pltpu.VMEM((1, cols), F32),
                pltpu.VMEM((HEAD + 8, cols), F32),
                pltpu.VMEM((1, cols), F32),
                pltpu.VMEM((HEAD + 8, cols), F32),
                pltpu.VMEM((own, cols), F32),
                pltpu.VMEM((own, cols), F32),
                pltpu.VMEM((own, cols), F32),
                pltpu.VMEM((own, cols), BF16),
                pltpu.VMEM((own, cols), BF16),
                pltpu.VMEM((own, cols), BF16),
                pltpu.VMEM((8, cols), F32),
                pltpu.VMEM((8, cols), F32),
                pltpu.VMEM((own, WIDE), F32),
                pltpu.SemaphoreType.DMA((2, n // 2, kvh)),
                pltpu.SemaphoreType.DMA((2, n // 2, kvh)),
                pltpu.SemaphoreType.DMA((SLOTS, 2)),
                pltpu.SemaphoreType.DMA((2, width // WIDE)),
                pltpu.SemaphoreType.DMA((2,)),
            ],
            compiler_params=pltpu.CompilerParams(collective_id=0, has_side_effects=True, vmem_limit_bytes=60 * 2**20),
            name="layer",
        )(x, gain, wq, wk, wv, wo)

    tokens, whole = P(("dp", "sp"), None), P(None, None)
    return jax.shard_map(
        step,
        mesh=mesh,
        in_specs=(tokens, P(None), whole, whole, whole, whole),
        out_specs=tokens,
        check_vma=False,
    )
```
